8 devices in a mesh: sp: 8 (over z, y, x, core).
Axes of the slice: x: 2, y: 2, z: 1, core: 2. Of those that a mesh axis runs over, the one named last changes fastest.
Arguments:
- x: bfloat16 [4096, 2048], P('sp')
- seg_ids: int32 [4096], P('sp')
- positions: int32 [4096], P('sp')
- grad_y: bfloat16 [4096, 2048], P('sp')
- norm1_gain: bfloat16 [2048], P('sp')
- w_q: bfloat16 [2048, 16, 128], P('sp')
- w_k: bfloat16 [2048, 16, 128], P('sp')
- w_v: bfloat16 [2048, 16, 128], P('sp')
- w_o: bfloat16 [16, 128, 2048], P('sp')
- norm2_gain: bfloat16 [2048], P('sp')
- w_gate: bfloat16 [2048, 5504], P('sp')
- w_up: bfloat16 [2048, 5504], P('sp')
- w_down: bfloat16 [5504, 2048], P('sp')
Outputs:
- output 1: bfloat16 [4096, 2048], P('sp')
- output 2: bfloat16 [4096, 2048], P('sp')
- output 3: float32 [2048], P('sp')
- output 4: float32 [2048, 16, 128], P('sp')
- output 5: float32 [2048, 16, 128], P('sp')
- output 6: float32 [2048, 16, 128], P('sp')
- output 7: float32 [16, 128, 2048], P('sp')
- output 8: float32 [2048], P('sp')
- output 9: float32 [2048, 5504], P('sp')
- output 10: float32 [2048, 5504], P('sp')
- output 11: float32 [5504, 2048], P('sp')
All inputs are finite; a program needn't handle non-finite values.
Results may differ from the reference program's by a relative error of at most 0.0156151.
Values are sent between devices in bfloat16 or wider.
A program may use at most 1 GiB of HBM per device.

```python
import jax
import jax.numpy as jnp
from jax import lax

D = 2048
HEADS = 16
KV_HEADS = 16
HEAD = 128
FF = 5504
SEQ = 4096
DOCS = 4
BLOCK = 256
NORM_EPS = 1e-5
ROPE_BASE = 10000.0
SCALE = HEAD ** -0.5


def doc_layout(key):
    cut_points = jax.random.permutation(key, SEQ - 1)[: DOCS - 1] + 1
    doc_starts = jnp.zeros((SEQ,), jnp.int32).at[cut_points].set(1)
    seg_ids = jnp.cumsum(doc_starts).astype(jnp.int32)
    tok_index = jnp.arange(SEQ, dtype=jnp.int32)
    first_index = lax.cummax(tok_index * doc_starts, axis=0)
    return seg_ids, (tok_index - first_index).astype(jnp.int32)


def normal_draw(key, shape, scale):
    return jax.random.normal(key, shape, jnp.float32) * scale


def setup_inputs(seed: int = 0) -> dict:
    keys = jax.random.split(jax.random.key(seed), 13)
    seg_ids, positions = doc_layout(keys[0])
    return {
        'x': normal_draw(keys[1], (SEQ, D), 1.0).astype(jnp.bfloat16),
        'seg_ids': seg_ids,
        'positions': positions,
        'grad_y': normal_draw(keys[2], (SEQ, D), 1.0).astype(jnp.bfloat16),
        'norm1_gain': (1.0 + normal_draw(keys[3], (D,), 0.5)).astype(jnp.bfloat16),
        'w_q': normal_draw(keys[4], (D, HEADS, HEAD), D ** -0.5).astype(jnp.bfloat16),
        'w_k': normal_draw(keys[5], (D, KV_HEADS, HEAD), D ** -0.5).astype(jnp.bfloat16),
        'w_v': normal_draw(keys[6], (D, KV_HEADS, HEAD), D ** -0.5).astype(jnp.bfloat16),
        'w_o': normal_draw(keys[7], (HEADS, HEAD, D), (HEADS * HEAD) ** -0.5).astype(jnp.bfloat16),
        'norm2_gain': (1.0 + normal_draw(keys[8], (D,), 0.5)).astype(jnp.bfloat16),
        'w_gate': normal_draw(keys[9], (D, FF), D ** -0.5).astype(jnp.bfloat16),
        'w_up': normal_draw(keys[10], (D, FF), D ** -0.5).astype(jnp.bfloat16),
        'w_down': normal_draw(keys[11], (FF, D), FF ** -0.5).astype(jnp.bfloat16),
    }


def to_bf16(t):
    return t.astype(jnp.bfloat16).astype(jnp.float32)


def rms_scale(t, gain):
    return t * lax.rsqrt(jnp.mean(t * t, axis=-1, keepdims=True) + NORM_EPS) * gain


def rope_tables(positions):
    half = HEAD // 2
    inv_freq = ROPE_BASE ** (-jnp.arange(half, dtype=jnp.float32) * 2.0 / HEAD)
    angle = positions.astype(jnp.float32)[:, None] * inv_freq[None, :]
    cos_t = jnp.cos(angle)
    sin_t = jnp.sin(angle)
    cos_full = jnp.concatenate([cos_t, cos_t], axis=-1)[:, None, :]
    sin_full = jnp.concatenate([sin_t, sin_t], axis=-1)[:, None, :]
    return cos_full, sin_full


def rotate(t, cos_full, sin_full):
    half = HEAD // 2
    return t * cos_full + jnp.concatenate([-t[..., half:], t[..., :half]], axis=-1) * sin_full


def head_attention(q_head, k_head, v_head, seg_ids):
    num_blocks = SEQ // BLOCK
    key_index = jnp.arange(SEQ)

    def one_block(block_args):
        q_block, block_id = block_args
        q_start = block_id * BLOCK
        q_index = q_start + jnp.arange(BLOCK)
        q_seg = lax.dynamic_slice(seg_ids, (q_start,), (BLOCK,))
        allowed = (key_index[None, :] <= q_index[:, None]) & (seg_ids[None, :] == q_seg[:, None])
        logits = jnp.dot(q_block, k_head.T, preferred_element_type=jnp.float32) * SCALE
        attn_probs = jax.nn.softmax(jnp.where(allowed, logits, -1e30), axis=-1)
        return to_bf16(jnp.dot(to_bf16(attn_probs), v_head, preferred_element_type=jnp.float32))

    attended = lax.map(jax.checkpoint(one_block), (q_head.reshape(num_blocks, BLOCK, HEAD), jnp.arange(num_blocks)))
    return attended.reshape(SEQ, HEAD)


def layer_forward(x_wide, seg_ids, positions, g_attn, w_q, w_k, w_v, w_o, g_mlp, w_gate, w_up, w_down):
    cos_full, sin_full = rope_tables(positions)
    u_norm = to_bf16(rms_scale(x_wide, g_attn))
    q_all = to_bf16(rotate(jnp.einsum('td,dhe->the', u_norm, w_q), cos_full, sin_full))
    k_all = to_bf16(rotate(jnp.einsum('td,dhe->the', u_norm, w_k), cos_full, sin_full))
    v_all = to_bf16(jnp.einsum('td,dhe->the', u_norm, w_v))
    group = HEADS // KV_HEADS
    k_rep = jnp.repeat(k_all, group, axis=1)
    v_rep = jnp.repeat(v_all, group, axis=1)
    attended = lax.map(lambda head_args: head_attention(head_args[0], head_args[1], head_args[2], seg_ids),
                       (q_all.transpose(1, 0, 2), k_rep.transpose(1, 0, 2), v_rep.transpose(1, 0, 2)))
    o_all = attended.transpose(1, 0, 2)
    h_res = to_bf16(x_wide + jnp.einsum('the,hed->td', o_all, w_o))
    z_norm = to_bf16(rms_scale(h_res, g_mlp))
    gate_pre = jnp.dot(z_norm, w_gate, preferred_element_type=jnp.float32)
    up_pre = jnp.dot(z_norm, w_up, preferred_element_type=jnp.float32)
    mlp_act = to_bf16(jax.nn.silu(gate_pre) * up_pre)
    return to_bf16(h_res + jnp.dot(mlp_act, w_down, preferred_element_type=jnp.float32))


def reference(x, seg_ids, positions, grad_y, norm1_gain, w_q, w_k, w_v, w_o, norm2_gain, w_gate, w_up, w_down):
    def forward(x_wide, g_attn, wq_full, wk_full, wv_full, wo_full, g_mlp, wgate_full, wup_full, wdown_full):
        return layer_forward(x_wide, seg_ids, positions, g_attn, wq_full, wk_full, wv_full, wo_full,
                             g_mlp, wgate_full, wup_full, wdown_full)

    primals = tuple(t.astype(jnp.float32) for t in (x, norm1_gain, w_q, w_k, w_v, w_o, norm2_gain, w_gate, w_up, w_down))
    y_out, pullback = jax.vjp(forward, *primals)
    grads = pullback(grad_y.astype(jnp.float32))
    return (y_out.astype(jnp.bfloat16), grads[0].astype(jnp.bfloat16), grads[1], grads[2], grads[3],
            grads[4], grads[5], grads[6], grads[7], grads[8], grads[9])
```

```python
import functools

import jax
import jax.numpy as jnp
from jax import lax
from jax.experimental import pallas as pl
from jax.experimental.pallas import tpu as pltpu
from jax.sharding import PartitionSpec as P

NORM_EPS = 1e-5
ROPE_BASE = 10000.0
BF = jnp.bfloat16
F32 = jnp.float32
BQ = 256
BK = 512
NEG = -1e30


def dot(a, b):
    return lax.dot_general(a, b, (((1,), (0,)), ((), ())), preferred_element_type=F32)


def dot_nt(a, b):
    return lax.dot_general(a, b, (((1,), (1,)), ((), ())), preferred_element_type=F32)


def dot_tn(a, b):
    return lax.dot_general(a, b, (((0,), (0,)), ((), ())), preferred_element_type=F32)


def allowed_block(i, j, start_row):
    kv = j * BK + lax.broadcasted_iota(jnp.int32, (BK, BQ), 0)
    qi = i * BQ + lax.broadcasted_iota(jnp.int32, (BK, BQ), 1)
    return (kv <= qi) & (kv >= start_row)


def attn_fwd_kernel(scale, lo_ref, q_ref, k_ref, vt_ref, start_ref, o_ref, lse_ref, s_scr):
    i = pl.program_id(1)
    lo = lo_ref[i]
    hi = (i * BQ + BQ - 1) // BK + 1
    q = q_ref[...]
    start_row = start_ref[0]

    def first(j, carry):
        m, l = carry
        kb = k_ref[pl.ds(pl.multiple_of(j * BK, BK), BK), :]
        s = dot_nt(kb, q) * scale
        s = jnp.where(allowed_block(i, j, start_row), s, NEG)
        s_scr[j] = s
        m_new = jnp.maximum(m, jnp.max(s, axis=0, keepdims=True))
        l = l * jnp.exp(m - m_new) + jnp.sum(jnp.exp(s - m_new), axis=0, keepdims=True)
        return m_new, l

    m, l = lax.fori_loop(lo, hi, first, (jnp.full((1, BQ), NEG, F32), jnp.zeros((1, BQ), F32)))
    lse = m + jnp.log(l)
    lse_ref[0, 0] = lse

    def second(j, acc):
        p = jnp.exp(s_scr[j] - lse).astype(BF)
        return acc + dot(vt_ref[:, pl.ds(pl.multiple_of(j * BK, BK), BK)], p)

    acc = lax.fori_loop(lo, hi, second, jnp.zeros((q.shape[1], BQ), F32))
    o_ref[...] = acc.T.astype(BF)


def attn_forward(q, k, vt, starts):
    tokens, width = q.shape
    hd = 128
    heads = width // hd
    nq = tokens // BQ
    lo = starts[::BQ] // BK
    grid_spec = pltpu.PrefetchScalarGridSpec(
        num_scalar_prefetch=1, grid=(heads, nq),
        in_specs=[pl.BlockSpec((BQ, hd), lambda h, i, *_: (i, h)),
                  pl.BlockSpec((tokens, hd), lambda h, i, *_: (0, h)),
                  pl.BlockSpec((hd, tokens), lambda h, i, *_: (h, 0)),
                  pl.BlockSpec((1, 1, BQ), lambda h, i, *_: (i, 0, 0))],
        out_specs=[pl.BlockSpec((BQ, hd), lambda h, i, *_: (i, h)),
                   pl.BlockSpec((1, 1, 1, BQ), lambda h, i, *_: (h, i, 0, 0))],
        scratch_shapes=[pltpu.VMEM((tokens // BK, BK, BQ), F32)])
    return pl.pallas_call(
        functools.partial(attn_fwd_kernel, hd ** -0.5),
        grid_spec=grid_spec,
        out_shape=[jax.ShapeDtypeStruct((tokens, width), BF),
                   jax.ShapeDtypeStruct((heads, nq, 1, BQ), F32)],
        compiler_params=pltpu.CompilerParams(dimension_semantics=("arbitrary", "arbitrary"),
                                             vmem_limit_bytes=40 * 1024 * 1024),
        cost_estimate=pl.CostEstimate(flops=25_000_000_000, bytes_accessed=10_000_000, transcendentals=10_000_000),
        name="attn_fwd",
    )(lo, q, k, vt, starts.reshape(nq, 1, BQ))


def attn_bwd_kernel(scale, lo_ref, q_ref, do_ref, k_ref, v_ref, kt_ref, lse_ref, delta_ref, start_ref,
                    dq_ref, dk_ref, dv_ref, dk_acc, dv_acc):
    i = pl.program_id(1)
    lo = lo_ref[i]
    hi = (i * BQ + BQ - 1) // BK + 1

    @pl.when(i == 0)
    def _():
        dk_acc[...] = jnp.zeros_like(dk_acc)
        dv_acc[...] = jnp.zeros_like(dv_acc)

    q = q_ref[...]
    do = do_ref[...]
    start_row = start_ref[0]
    lse = lse_ref[0, 0]
    delta = delta_ref[0, 0]

    def body(j, dqt):
        rows = pl.ds(pl.multiple_of(j * BK, BK), BK)
        s = dot_nt(k_ref[rows, :], q) * scale
        p = jnp.where(allowed_block(i, j, start_row), jnp.exp(s - lse), 0.0)
        dv_acc[rows, :] += dot(p.astype(BF), do)
        dp = dot_nt(v_ref[rows, :], do).astype(BF).astype(F32)
        ds = (p * (dp - delta) * scale).astype(BF)
        dk_acc[rows, :] += dot(ds, q)
        return dqt + dot(kt_ref[:, rows], ds)

    dqt = lax.fori_loop(lo, hi, body, jnp.zeros((q.shape[1], BQ), F32))
    dq_ref[...] = dqt.T.astype(BF)

    @pl.when(i == pl.num_programs(1) - 1)
    def _():
        dk_ref[...] = dk_acc[...].astype(BF)
        dv_ref[...] = dv_acc[...].astype(BF)


def attn_backward(q, k, v, kt, grad_o, lse, delta, starts):
    tokens, width = q.shape
    hd = 128
    heads = width // hd
    nq = tokens // BQ
    lo = starts[::BQ] // BK
    row = pl.BlockSpec((BQ, hd), lambda h, i, *_: (i, h))
    col = pl.BlockSpec((tokens, hd), lambda h, i, *_: (0, h))
    stat = pl.BlockSpec((1, 1, 1, BQ), lambda h, i, *_: (h, i, 0, 0))
    grid_spec = pltpu.PrefetchScalarGridSpec(
        num_scalar_prefetch=1, grid=(heads, nq),
        in_specs=[row, row, col, col,
                  pl.BlockSpec((hd, tokens), lambda h, i, *_: (h, 0)),
                  stat, stat,
                  pl.BlockSpec((1, 1, BQ), lambda h, i, *_: (i, 0, 0))],
        out_specs=[row, col, col],
        scratch_shapes=[pltpu.VMEM((tokens, hd), F32), pltpu.VMEM((tokens, hd), F32)])
    out = jax.ShapeDtypeStruct((tokens, width), BF)
    return pl.pallas_call(
        functools.partial(attn_bwd_kernel, hd ** -0.5),
        grid_spec=grid_spec,
        out_shape=[out, out, out],
        compiler_params=pltpu.CompilerParams(dimension_semantics=("arbitrary", "arbitrary"),
                                             vmem_limit_bytes=40 * 1024 * 1024),
        cost_estimate=pl.CostEstimate(flops=60_000_000_000, bytes_accessed=20_000_000, transcendentals=10_000_000),
        name="attn_bwd",
    )(lo, q, grad_o, k, v, kt, lse, delta, starts.reshape(nq, 1, BQ))


def rms_back(grad_out, normed, inv_rms):
    mean_term = jnp.mean(grad_out * normed, axis=-1, keepdims=True)
    return inv_rms * (grad_out - normed * mean_term)


def solution(mesh):
    row_spec = P('sp', None)
    cube_spec = P('sp', None, None)
    vec_spec = P('sp')
    n = mesh.shape['sp']

    def gather(t):
        return lax.all_gather(t, 'sp', axis=0, tiled=True)

    def swap(t, mask):
        return lax.ppermute(t, 'sp', [(d, d ^ mask) for d in range(n)])

    def pick(t, index, axis=0):
        return lax.dynamic_index_in_dim(t, index, axis, keepdims=False)

    def halves(mine, other, pos):
        first = jnp.where(pos == 0, mine, other)
        second = jnp.where(pos == 0, other, mine)
        return jnp.concatenate([first, second], axis=0)

    def local_layer(x, seg_ids, positions, grad_y, norm1_gain, w_q, w_k, w_v, w_o, norm2_gain, w_gate, w_up, w_down):
        tl, d = x.shape
        tokens = tl * n
        dr = w_gate.shape[0]
        ff = w_gate.shape[1]
        fr = w_down.shape[0]
        hw = d // n
        head_dim = w_q.shape[2]
        me = lax.axis_index('sp')
        yy = me // 4
        qq = me % 4
        xx = qq // 2
        cc = qq % 2

        small = gather(jnp.concatenate([norm1_gain.astype(F32), norm2_gain.astype(F32),
                                        positions.astype(F32)])[None])
        gain1 = small[:, :dr].reshape(-1)
        gain2 = small[:, dr:2 * dr].reshape(-1)
        pos_all = small[:, 2 * dr:].reshape(-1)
        starts = jnp.arange(tokens, dtype=jnp.int32) - pos_all.astype(jnp.int32)

        half = head_dim // 2
        inv_freq = ROPE_BASE ** (-jnp.arange(half, dtype=F32) * 2.0 / head_dim)
        angle = pos_all[:, None] * inv_freq[None, :]
        cos_t, sin_t = jnp.cos(angle), jnp.sin(angle)
        cos_full = jnp.concatenate([cos_t] * 4, axis=-1)
        sin_full = jnp.concatenate([sin_t] * 4, axis=-1)

        def rotate_half(t):
            parts = []
            for h in range(t.shape[-1] // head_dim):
                lo = t[:, h * head_dim:h * head_dim + half]
                hi = t[:, h * head_dim + half:(h + 1) * head_dim]
                parts += [-hi, lo]
            return jnp.concatenate(parts, axis=-1)

        def rope_apply(t):
            return t * cos_full + rotate_half(t) * sin_full

        def rope_back(t):
            return t * cos_full - rotate_half(t) * sin_full

        x_wide = x.astype(F32)
        inv_rms1 = lax.rsqrt(jnp.mean(x_wide * x_wide, axis=-1, keepdims=True) + NORM_EPS)
        normed1 = x_wide * inv_rms1
        u_norm = (normed1 * gain1).astype(BF)
        u_all = gather(u_norm)

        def quarter_rows(w4):
            blocks = [pick(w4, qq)] + [swap(pick(w4, qq ^ m), m) for m in (1, 2, 3)]
            out = jnp.zeros((4,) + w4.shape[1:], w4.dtype)
            for m in range(4):
                out = lax.dynamic_update_slice(out, blocks[m][None], (qq ^ m, 0, 0))
            return out.reshape(4 * dr, -1)

        wqkv = jnp.stack([w.reshape(dr, 2, 4, hw) for w in (w_q, w_k, w_v)], axis=1)
        wqkv = wqkv.transpose(3, 0, 2, 1, 4).reshape(4, dr, 6 * hw)
        s_qkv = quarter_rows(wqkv)
        s_own = lax.dynamic_slice_in_dim(s_qkv, yy * 3 * hw, 3 * hw, 1)
        s_oth = lax.dynamic_slice_in_dim(s_qkv, (1 - yy) * 3 * hw, 3 * hw, 1)
        w_own = halves(s_own, swap(s_oth, 4), yy)

        qkv = dot(u_all, w_own)
        q = rope_apply(qkv[:, :hw]).astype(BF)
        k = rope_apply(qkv[:, hw:2 * hw]).astype(BF)
        v = qkv[:, 2 * hw:].astype(BF)
        o, lse = attn_forward(q, k, v.T, starts)

        o_loc = lax.all_to_all(o, 'sp', 0, 1, tiled=True)
        wo_own = w_o.reshape(hw, d)
        wo_full = gather(wo_own)
        gy_all = gather(grad_y)

        def ff_quarter(w):
            w4 = w.reshape(dr, 2, 4, fr).transpose(2, 0, 1, 3).reshape(4, dr, 2 * fr)
            mine = quarter_rows(w4)
            return halves(mine, swap(mine, 4), yy)

        wd_quarter = halves(w_down, swap(w_down, 4), yy)
        wg_quarter = ff_quarter(w_gate)
        wu_quarter = ff_quarter(w_up)

        h_res = (x_wide + dot(o_loc, wo_full)).astype(BF)
        h_wide = h_res.astype(F32)
        inv_rms2 = lax.rsqrt(jnp.mean(h_wide * h_wide, axis=-1, keepdims=True) + NORM_EPS)
        normed2 = h_wide * inv_rms2
        z_norm = (normed2 * gain2).astype(BF)
        z_all = gather(z_norm)

        grad_act = dot_nt(gy_all, wd_quarter).astype(BF).astype(F32)
        gate_pre = dot(z_all, wg_quarter)
        up_pre = dot(z_all, wu_quarter)
        gate_sig = jax.nn.sigmoid(gate_pre)
        gate_act = gate_pre * gate_sig
        mlp_act = (gate_act * up_pre).astype(BF)
        grad_gate = (grad_act * up_pre * gate_sig * (1.0 + gate_pre * (1.0 - gate_sig))).astype(BF)
        grad_up = (grad_act * gate_act).astype(BF)

        def token_half(t):
            return lax.dynamic_slice_in_dim(t, yy * 4 * tl, 4 * tl, 0)

        def quarter_sum(part):
            part = part.reshape(2, 2, tl, d)
            kept = pick(part, cc, 1) + swap(pick(part, 1 - cc, 1), 1)
            return pick(kept, xx) + swap(pick(kept, 1 - xx), 2)

        gz = quarter_sum(dot_nt(token_half(grad_gate), wg_quarter) + dot_nt(token_half(grad_up), wu_quarter))
        gz = gz.astype(BF).astype(F32)
        grad_gain2 = jnp.sum(gz * normed2, axis=0)
        grad_h = (grad_y.astype(F32) + rms_back(gz * gain2, normed2, inv_rms2)).astype(BF)
        gh_all = gather(grad_h)

        y = (h_wide + quarter_sum(dot(token_half(mlp_act), wd_quarter))).astype(BF)

        z_cols = lax.dynamic_slice_in_dim(z_all, yy * 4 * dr, 4 * dr, 1)

        def spread_rows(g):
            g4 = g.reshape(4, dr, 2 * fr)
            blocks = [pick(g4, qq)] + [swap(pick(g4, qq ^ m), m) for m in (1, 2, 3)]
            out = jnp.zeros((4, dr, 2 * fr), F32)
            for m in range(4):
                out = lax.dynamic_update_slice(out, blocks[m][None], (qq ^ m, 0, 0))
            return out.reshape(4, dr, 2, fr).transpose(1, 2, 0, 3).reshape(dr, ff)

        grad_wgate = spread_rows(dot_tn(z_cols, grad_gate))
        grad_wup = spread_rows(dot_tn(z_cols, grad_up))
        grad_wdown = dot_tn(lax.dynamic_slice_in_dim(mlp_act, yy * fr, fr, 1), gy_all)

        grad_o = dot_nt(gh_all, wo_own).astype(BF)
        grad_wo = dot_tn(o, gh_all)
        delta = jnp.sum((grad_o.astype(F32) * o.astype(F32)).reshape(tokens, -1, head_dim), axis=-1)
        delta = delta.T.reshape(lse.shape)
        dq, dk, dv = attn_backward(q, k, v, k.T, grad_o, lse, delta, starts)
        dq_pre = rope_back(dq.astype(F32)).astype(BF)
        dk_pre = rope_back(dk.astype(F32)).astype(BF)
        dqkv = jnp.concatenate([dq_pre, dk_pre, dv], axis=1)

        d_own = token_half(dqkv)
        d_oth = swap(lax.dynamic_slice_in_dim(dqkv, (1 - yy) * 4 * tl, 4 * tl, 0), 4)
        w_oth = halves(s_oth, swap(s_own, 4), yy)
        gu = quarter_sum(dot_nt(d_own, w_own) + dot_nt(d_oth, w_oth))
        gu = gu.astype(BF).astype(F32)

        def spread_heads(g):
            return lax.all_to_all(g, 'sp', 0, 1, tiled=True)

        grad_wq = spread_heads(dot_tn(u_all, dq_pre))
        grad_wk = spread_heads(dot_tn(u_all, dk_pre))
        grad_wv = spread_heads(dot_tn(u_all, dv))

        grad_gain1 = jnp.sum(gu * normed1, axis=0)
        grad_x = (grad_h.astype(F32) + rms_back(gu * gain1, normed1, inv_rms1)).astype(BF)
        gains = jnp.stack([grad_gain1.reshape(n, dr), grad_gain2.reshape(n, dr)], axis=1)
        gains = jnp.sum(lax.all_to_all(gains, 'sp', 0, 0, tiled=True), axis=0)
        return (y, grad_x, gains[0], grad_wq.reshape(w_q.shape), grad_wk.reshape(w_k.shape),
                grad_wv.reshape(w_v.shape), grad_wo.reshape(w_o.shape), gains[1], grad_wgate, grad_wup, grad_wdown)

    return jax.shard_map(
        local_layer, mesh=mesh,
        in_specs=(row_spec, vec_spec, vec_spec, row_spec, vec_spec, cube_spec, cube_spec, cube_spec, cube_spec,
                  vec_spec, row_spec, row_spec, row_spec),
        out_specs=(row_spec, row_spec, vec_spec, cube_spec, cube_spec, cube_spec, cube_spec, vec_spec,
                   row_spec, row_spec, row_spec),
        check_vma=False)
```

```python
import functools

import jax
import jax.numpy as jnp
from jax import lax
from jax.experimental import pallas as pl
from jax.experimental.pallas import tpu as pltpu
from jax.sharding import PartitionSpec as P

NORM_EPS = 1e-5
ROPE_BASE = 10000.0
BF = jnp.bfloat16
F32 = jnp.float32
HD = 128
BT = 256
BQ = 256
BK = 512
NEG = -1e30
SIB, XN, YN = 1, 2, 4


def dot(a, b):
    return lax.dot_general(a, b, (((1,), (0,)), ((), ())), preferred_element_type=F32)


def dot_nt(a, b):
    return lax.dot_general(a, b, (((1,), (1,)), ((), ())), preferred_element_type=F32)


def dot_tn(a, b):
    return lax.dot_general(a, b, (((0,), (0,)), ((), ())), preferred_element_type=F32)


def head_cols(h):
    return slice(h * HD, (h + 1) * HD)


def qkv_kernel(x_ref, gain_ref, w_ref, cos_ref, sin_ref, u_ref, q_ref, k_ref, v_ref, kt_ref, vt_ref):
    xw = x_ref[...].astype(F32)
    inv = lax.rsqrt(jnp.mean(xw * xw, axis=-1, keepdims=True) + NORM_EPS)
    u = (xw * inv * gain_ref[...]).astype(BF)
    u_ref[...] = u
    cos, sin = cos_ref[...], sin_ref[...]
    width = q_ref.shape[1]
    for part, ref in ((0, q_ref), (1, k_ref), (2, v_ref)):
        t = dot(u, w_ref[:, part * width:(part + 1) * width])
        for h in range(width // HD):
            th = t[:, head_cols(h)]
            if part < 2:
                th = th * cos + pltpu.roll(th, HD // 2, 1) * sin
            tb = th.astype(BF)
            ref[:, head_cols(h)] = tb
            if part == 1:
                kt_ref[head_cols(h), :] = tb.astype(F32).T.astype(BF)
            if part == 2:
                vt_ref[head_cols(h), :] = tb.astype(F32).T.astype(BF)


def qkv_project(x_all, gain, w, cos, sin):
    tokens, d = x_all.shape
    width = w.shape[1] // 3
    row = lambda k: pl.BlockSpec((BT, k), lambda i: (i, 0))
    full = lambda a: pl.BlockSpec(a.shape, lambda i: (0, 0))
    col = pl.BlockSpec((width, BT), lambda i: (0, i))
    tok = jax.ShapeDtypeStruct((tokens, width), BF)
    tra = jax.ShapeDtypeStruct((width, tokens), BF)
    return pl.pallas_call(
        qkv_kernel, grid=(tokens // BT,),
        in_specs=[row(d), full(gain), full(w), row(HD), row(HD)],
        out_specs=[row(d), row(width), row(width), row(width), col, col],
        out_shape=[jax.ShapeDtypeStruct((tokens, d), BF), tok, tok, tok, tra, tra],
        compiler_params=pltpu.CompilerParams(dimension_semantics=("arbitrary",), vmem_limit_bytes=40 * 1024 * 1024),
        cost_estimate=pl.CostEstimate(flops=2 * tokens * d * 3 * width, bytes_accessed=50_000_000, transcendentals=0),
        name="qkv_proj",
    )(x_all, gain, w, cos, sin)


def fold(t, op):
    return op(t.reshape(t.shape[0] // 8, 8, t.shape[1]), axis=0)


def block_allowed(i, j, start_row):
    kv = lax.broadcasted_iota(jnp.int32, (BK, BQ), 0)
    top = i * BQ - j * BK + lax.broadcasted_iota(jnp.int32, (1, BQ), 1)
    return (kv <= top) & (kv >= start_row - j * BK)


def attn_fwd_kernel(scale, heads, lo_ref, q_ref, k_ref, vt_ref, start_ref, o_ref, lse_ref, s_scr):
    i = pl.program_id(0)
    lo = lo_ref[i]
    hi = (i * BQ + BQ - 1) // BK + 1
    start_row = start_ref[0]
    zero = tuple(jnp.zeros((8, BQ), F32) for _ in range(heads))

    def logits(j, ms):
        rows = pl.ds(pl.multiple_of(j * BK, BK), BK)
        ok = block_allowed(i, j, start_row)
        out = []
        for h in range(heads):
            s = dot_nt(k_ref[rows, head_cols(h)], q_ref[:, head_cols(h)]) * scale
            s = jnp.where(ok, s, NEG)
            s_scr[h, j] = s
            out.append(jnp.maximum(ms[h], fold(s, jnp.max)))
        return tuple(out)

    ms = lax.fori_loop(lo, hi, logits, tuple(z + NEG for z in zero))
    ms = [jnp.max(m, axis=0, keepdims=True) for m in ms]

    def exps(j, ls):
        out = []
        for h in range(heads):
            e = jnp.exp(s_scr[h, j] - ms[h])
            s_scr[h, j] = e
            out.append(ls[h] + fold(e, jnp.sum))
        return tuple(out)

    ls = lax.fori_loop(lo, hi, exps, zero)
    ls = [jnp.sum(l, axis=0, keepdims=True) for l in ls]
    inv = [1.0 / l for l in ls]
    for h in range(heads):
        lse_ref[0, h:h + 1, :] = ms[h] + jnp.log(ls[h])

    def values(j, accs):
        rows = pl.ds(pl.multiple_of(j * BK, BK), BK)
        return tuple(accs[h] + dot(vt_ref[head_cols(h), rows], (s_scr[h, j] * inv[h]).astype(BF))
                     for h in range(heads))

    accs = lax.fori_loop(lo, hi, values, tuple(jnp.zeros((HD, BQ), F32) for _ in range(heads)))
    for h in range(heads):
        o_ref[:, head_cols(h)] = accs[h].T.astype(BF)


def attn_forward(q, k, vt, starts):
    tokens, width = q.shape
    heads = width // HD
    nq = tokens // BQ
    grid_spec = pltpu.PrefetchScalarGridSpec(
        num_scalar_prefetch=1, grid=(nq,),
        in_specs=[pl.BlockSpec((BQ, width), lambda i, *_: (i, 0)),
                  pl.BlockSpec((tokens, width), lambda i, *_: (0, 0)),
                  pl.BlockSpec((width, tokens), lambda i, *_: (0, 0)),
                  pl.BlockSpec((1, 1, BQ), lambda i, *_: (i, 0, 0))],
        out_specs=[pl.BlockSpec((BQ, width), lambda i, *_: (i, 0)),
                   pl.BlockSpec((1, heads, BQ), lambda i, *_: (i, 0, 0))],
        scratch_shapes=[pltpu.VMEM((heads, tokens // BK, BK, BQ), F32)])
    return pl.pallas_call(
        functools.partial(attn_fwd_kernel, HD ** -0.5, heads),
        grid_spec=grid_spec,
        out_shape=[jax.ShapeDtypeStruct((tokens, width), BF),
                   jax.ShapeDtypeStruct((nq, heads, BQ), F32)],
        compiler_params=pltpu.CompilerParams(dimension_semantics=("arbitrary",), vmem_limit_bytes=40 * 1024 * 1024),
        cost_estimate=pl.CostEstimate(flops=40_000_000_000, bytes_accessed=10_000_000, transcendentals=10_000_000),
        name="attn_fwd",
    )(starts[::BQ] // BK, q, k, vt, starts.reshape(nq, 1, BQ))


def attn_bwd_kernel(scale, heads, lo_ref, q_ref, do_ref, o_ref, k_ref, v_ref, kt_ref, lse_ref, start_ref,
                    cosq_ref, sinq_ref, cos_ref, sin_ref, dq_ref, dk_ref, dv_ref, dk_acc, dv_acc):
    i = pl.program_id(0)
    lo = lo_ref[i]
    hi = (i * BQ + BQ - 1) // BK + 1

    def rope_back(t, cos, sin):
        return (t * cos - pltpu.roll(t, HD // 2, 1) * sin).astype(BF)

    @pl.when(i == 0)
    def _():
        dk_acc[...] = jnp.zeros_like(dk_acc)
        dv_acc[...] = jnp.zeros_like(dv_acc)

    start_row = start_ref[0]
    delta = []
    for h in range(heads):
        prod = do_ref[:, head_cols(h)].astype(F32) * o_ref[:, head_cols(h)].astype(F32)
        delta.append(jnp.sum(prod.T, axis=0, keepdims=True))

    def body(j, dqts):
        rows = pl.ds(pl.multiple_of(j * BK, BK), BK)
        ok = block_allowed(i, j, start_row)
        out = []
        for h in range(heads):
            c = head_cols(h)
            q = q_ref[:, c]
            do = do_ref[:, c]
            s = dot_nt(k_ref[rows, c], q) * scale
            p = jnp.where(ok, jnp.exp(s - lse_ref[0, h:h + 1, :]), 0.0)
            dv_acc[rows, c] += dot(p.astype(BF), do)
            dp = dot_nt(v_ref[rows, c], do).astype(BF).astype(F32)
            ds = (p * (dp - delta[h]) * scale).astype(BF)
            dk_acc[rows, c] += dot(ds, q)
            out.append(dqts[h] + dot(kt_ref[c, rows], ds))
        return tuple(out)

    dqts = lax.fori_loop(lo, hi, body, tuple(jnp.zeros((HD, BQ), F32) for _ in range(heads)))
    for h in range(heads):
        dq = dqts[h].T.astype(BF).astype(F32)
        dq_ref[:, head_cols(h)] = rope_back(dq, cosq_ref[...], sinq_ref[...])

    @pl.when(i == pl.num_programs(0) - 1)
    def _():
        def finish(b, carry):
            rows = pl.ds(pl.multiple_of(b * BK, BK), BK)
            for h in range(heads):
                c = head_cols(h)
                dk = dk_acc[rows, c].astype(BF).astype(F32)
                dk_ref[rows, c] = rope_back(dk, cos_ref[rows, :], sin_ref[rows, :])
                dv_ref[rows, c] = dv_acc[rows, c].astype(BF)
            return carry

        lax.fori_loop(0, dk_acc.shape[0] // BK, finish, 0)


def attn_backward(q, k, v, kt, grad_o, o, lse, starts, cos, sin):
    tokens, width = q.shape
    heads = width // HD
    nq = tokens // BQ
    row = lambda w: pl.BlockSpec((BQ, w), lambda i, *_: (i, 0))
    full = lambda a: pl.BlockSpec(a, lambda i, *_: (0, 0))
    stat = lambda r: pl.BlockSpec((1, r, BQ), lambda i, *_: (i, 0, 0))
    grid_spec = pltpu.PrefetchScalarGridSpec(
        num_scalar_prefetch=1, grid=(nq,),
        in_specs=[row(width), row(width), row(width), full((tokens, width)), full((tokens, width)),
                  full((width, tokens)), stat(heads), stat(1), row(HD), row(HD), full((tokens, HD)), full((tokens, HD))],
        out_specs=[row(width), full((tokens, width)), full((tokens, width))],
        scratch_shapes=[pltpu.VMEM((tokens, width), F32), pltpu.VMEM((tokens, width), F32)])
    out = jax.ShapeDtypeStruct((tokens, width), BF)
    return pl.pallas_call(
        functools.partial(attn_bwd_kernel, HD ** -0.5, heads),
        grid_spec=grid_spec,
        out_shape=[out, out, out],
        compiler_params=pltpu.CompilerParams(dimension_semantics=("arbitrary",), vmem_limit_bytes=48 * 1024 * 1024),
        cost_estimate=pl.CostEstimate(flops=60_000_000_000, bytes_accessed=20_000_000, transcendentals=10_000_000),
        name="attn_bwd",
    )(starts[::BQ] // BK, q, grad_o, o, k, v, kt, lse, starts.reshape(nq, 1, BQ), cos, sin, cos, sin)


def rms_back(grad_out, normed, inv_rms):
    mean_term = jnp.mean(grad_out * normed, axis=-1, keepdims=True)
    return inv_rms * (grad_out - normed * mean_term)


def solution(mesh):
    row_spec = P('sp', None)
    cube_spec = P('sp', None, None)
    vec_spec = P('sp')
    n = mesh.shape['sp']
    same_y = [list(range(n // 2)), list(range(n // 2, n))]

    def gather(t):
        return lax.all_gather(t, 'sp', axis=0, tiled=True)

    def swap(t, mask):
        return lax.ppermute(t, 'sp', [(d, d ^ mask) for d in range(n)])

    def local_layer(x, seg_ids, positions, grad_y, norm1_gain, w_q, w_k, w_v, w_o, norm2_gain, w_gate, w_up, w_down):
        tl, d = x.shape
        tokens = tl * n
        dr = w_gate.shape[0]
        ff = w_gate.shape[1]
        fr = w_down.shape[0]
        hw = d // n
        me = lax.axis_index('sp')
        yy = me // 4

        with jax.named_scope("gx"):
            x_all = gather(x)
        with jax.named_scope("gsmall"):
            small = gather(jnp.concatenate([norm1_gain.astype(F32), norm2_gain.astype(F32),
                                            positions.astype(F32)])[None])
        gain1 = small[:, :dr].reshape(1, -1)
        gain2 = small[:, dr:2 * dr].reshape(1, -1)
        pos_all = small[:, 2 * dr:].reshape(-1)
        starts = jnp.arange(tokens, dtype=jnp.int32) - pos_all.astype(jnp.int32)

        half = HD // 2
        inv_freq = ROPE_BASE ** (-jnp.arange(half, dtype=F32) * 2.0 / HD)
        angle = pos_all[:, None] * inv_freq[None, :]
        cos_t, sin_t = jnp.cos(angle), jnp.sin(angle)
        cos_full = jnp.concatenate([cos_t, cos_t], axis=-1)
        sin_full = jnp.concatenate([-sin_t, sin_t], axis=-1)

        with jax.named_scope("wqkv"):
            wqkv = jnp.stack([w.reshape(dr, n, hw) for w in (w_q, w_k, w_v)], axis=2).reshape(dr, -1)
            w_own = lax.all_to_all(wqkv, 'sp', 1, 0, tiled=True)

        def half_tokens(t, name):
            with jax.named_scope(name + "_x"):
                pair = jnp.concatenate([t, swap(t, XN)], axis=0)
            with jax.named_scope(name + "_s"):
                return pair, jnp.concatenate([pair, swap(pair, SIB)], axis=0)

        def other_half(pair, name):
            with jax.named_scope(name + "_y"):
                far = swap(pair, YN)
            with jax.named_scope(name + "_ys"):
                return jnp.concatenate([far, swap(far, SIB)], axis=0)

        gy_pair, gy_half = half_tokens(grad_y, "gy")

        with jax.named_scope("wd"):
            far = swap(w_down, YN)
            wd_quarter = jnp.concatenate([jnp.where(yy == 0, w_down, far), jnp.where(yy == 0, far, w_down)], axis=0)

        def ff_quarter(w):
            w4 = w.reshape(dr, 2, 4, fr).transpose(0, 2, 1, 3).reshape(dr, 4 * 2 * fr)
            return lax.all_to_all(jnp.concatenate([w4, w4], axis=1), 'sp', 1, 0, tiled=True)

        with jax.named_scope("wg"):
            wg_quarter = ff_quarter(w_gate)
        with jax.named_scope("wu"):
            wu_quarter = ff_quarter(w_up)

        with jax.named_scope("qkv"):
            u_all, q, k, v, kt, vt = qkv_project(x_all, gain1, w_own, cos_full, sin_full)
        with jax.named_scope("attnf"):
            o, lse = attn_forward(q, k, vt, starts)

        with jax.named_scope("oloc"):
            o_loc = lax.all_to_all(o, 'sp', 0, 1, tiled=True)
        wo_own = w_o.reshape(hw, d)
        with jax.named_scope("gwo"):
            wo_full = gather(wo_own)
        x_wide = x.astype(F32)
        with jax.named_scope("oproj"):
            h_res = (x_wide + dot(o_loc, wo_full)).astype(BF)
        h_wide = h_res.astype(F32)
        inv_rms2 = lax.rsqrt(jnp.mean(h_wide * h_wide, axis=-1, keepdims=True) + NORM_EPS)
        normed2 = h_wide * inv_rms2
        z_norm = (normed2 * gain2).astype(BF)
        z_pair, z_half = half_tokens(z_norm, "z")

        def mlp(z, gy):
            grad_act = dot_nt(gy, wd_quarter).astype(BF).astype(F32)
            gate_pre = dot(z, wg_quarter)
            up_pre = dot(z, wu_quarter)
            gate_sig = jax.nn.sigmoid(gate_pre)
            gate_act = gate_pre * gate_sig
            mlp_act = (gate_act * up_pre).astype(BF)
            grad_gate = (grad_act * up_pre * gate_sig * (1.0 + gate_pre * (1.0 - gate_sig))).astype(BF)
            grad_up = (grad_act * gate_act).astype(BF)
            return mlp_act, grad_gate, grad_up

        def quarter_sum(near, far, name):
            with jax.named_scope(name + "_s"):
                kept = near + swap(far, SIB)
            with jax.named_scope(name + "_x"):
                return kept[:tl] + swap(kept[tl:], XN)

        with jax.named_scope("mlp1"):
            m1, gg1, gu1 = mlp(z_half, gy_half)
        with jax.named_scope("gzdot"):
            gz_far = dot_nt(gg1[2 * tl:], wg_quarter) + dot_nt(gu1[2 * tl:], wu_quarter)
            gz_near = dot_nt(gg1[:2 * tl], wg_quarter) + dot_nt(gu1[:2 * tl], wu_quarter)
        gz = quarter_sum(gz_near, gz_far, "gz")
        gz = gz.astype(BF).astype(F32)
        grad_gain2 = jnp.sum(gz * normed2, axis=0)
        grad_h = (grad_y.astype(F32) + rms_back(gz * gain2, normed2, inv_rms2)).astype(BF)
        with jax.named_scope("ggh"):
            gh_all = gather(grad_h)

        with jax.named_scope("ydot"):
            y_far = dot(m1[2 * tl:], wd_quarter)
            y_near = dot(m1[:2 * tl], wd_quarter)
        y = (h_wide + quarter_sum(y_near, y_far, "y")).astype(BF)

        z_oth = other_half(z_pair, "zo")
        gy_oth = other_half(gy_pair, "gyo")
        with jax.named_scope("mlp2"):
            m2, gg2, gu2 = mlp(z_oth, gy_oth)

        def cols(t, width, start):
            return lax.dynamic_slice_in_dim(t, start, width, 1)

        zc1 = cols(z_half, 4 * dr, yy * 4 * dr)
        zc2 = cols(z_oth, 4 * dr, yy * 4 * dr)

        def spread_rows(g):
            out = lax.all_to_all(g, 'sp', 0, 1, axis_index_groups=same_y, tiled=True)
            return out.reshape(dr, 4, 2, fr).transpose(0, 2, 1, 3).reshape(dr, ff)

        with jax.named_scope("gwg"):
            grad_wgate = spread_rows(dot_tn(zc1, gg1) + dot_tn(zc2, gg2))
        with jax.named_scope("gwu"):
            grad_wup = spread_rows(dot_tn(zc1, gu1) + dot_tn(zc2, gu2))
        with jax.named_scope("gwd"):
            grad_wdown = dot_tn(cols(m1, fr, yy * fr), gy_half) + dot_tn(cols(m2, fr, yy * fr), gy_oth)

        with jax.named_scope("gradodot"):
            grad_o = dot_nt(gh_all, wo_own).astype(BF)
        with jax.named_scope("attnb"):
            dq, dk, dv = attn_backward(q, k, v, kt, grad_o, o, lse, starts, cos_full, sin_full)
        dqkv = jnp.concatenate([dq, dk, dv], axis=1)

        def token_blocks(masks):
            return jnp.concatenate([lax.dynamic_slice_in_dim(dqkv, (me ^ m) * tl, tl, 0) for m in masks], axis=0)

        with jax.named_scope("woth"):
            w_oth = swap(w_own, YN)
        with jax.named_scope("doth"):
            d_oth = swap(token_blocks((4, 6, 5, 7)), YN)
        d_own = token_blocks((0, 2, 1, 3))
        with jax.named_scope("gudot"):
            u_far = dot_nt(d_own[2 * tl:], w_own) + dot_nt(d_oth[2 * tl:], w_oth)
            u_near = dot_nt(d_own[:2 * tl], w_own) + dot_nt(d_oth[:2 * tl], w_oth)
        gu = quarter_sum(u_near, u_far, "gu")
        gu = gu.astype(BF).astype(F32)

        with jax.named_scope("gwo"):
            grad_wo = dot_tn(o, gh_all)

        def spread_heads(g):
            return lax.all_to_all(g, 'sp', 0, 1, tiled=True)

        with jax.named_scope("gwqkv"):
            grad_wq = spread_heads(dot_tn(u_all, dq))
            grad_wk = spread_heads(dot_tn(u_all, dk))
            grad_wv = spread_heads(dot_tn(u_all, dv))

        inv_rms1 = lax.rsqrt(jnp.mean(x_wide * x_wide, axis=-1, keepdims=True) + NORM_EPS)
        normed1 = x_wide * inv_rms1
        grad_gain1 = jnp.sum(gu * normed1, axis=0)
        grad_x = (grad_h.astype(F32) + rms_back(gu * gain1, normed1, inv_rms1)).astype(BF)
        with jax.named_scope("gains"):
            gains = jnp.stack([grad_gain1.reshape(n, dr), grad_gain2.reshape(n, dr)], axis=1)
            gains = jnp.sum(lax.all_to_all(gains, 'sp', 0, 0, tiled=True), axis=0)
        return (y, grad_x, gains[0], grad_wq.reshape(w_q.shape), grad_wk.reshape(w_k.shape),
                grad_wv.reshape(w_v.shape), grad_wo.reshape(w_o.shape), gains[1], grad_wgate, grad_wup, grad_wdown)

    return jax.shard_map(
        local_layer, mesh=mesh,
        in_specs=(row_spec, vec_spec, vec_spec, row_spec, vec_spec, cube_spec, cube_spec, cube_spec, cube_spec,
                  vec_spec, row_spec, row_spec, row_spec),
        out_specs=(row_spec, row_spec, vec_spec, cube_spec, cube_spec, cube_spec, cube_spec, vec_spec,
                   row_spec, row_spec, row_spec),
        check_vma=False)
```
